32 devices in a mesh: row: 4 (over y, core), col: 8 (over z, x).
Axes of the slice: x: 2, y: 2, z: 4, core: 2. Of those that a mesh axis runs over, the one named last changes fastest.
Arguments:
- inner_base: bfloat16 [4, 1, 2, 4096, 14336], P(None, None, None, 'row', 'col'), may hold values from -250 to 250
- inner_left: bfloat16 [4, 1, 2, 4096, 16], P(None, None, None, ('row', 'col')), may hold values from -6 to 6
- inner_right: bfloat16 [4, 1, 2, 16, 14336], P(None, None, None, 'row', 'col'), may hold values from -12 to 12
- inner_mag: float32 [4, 1, 2, 14336], P(None, None, None, 'col'), may hold values from 512 to 2048
- outer_base: bfloat16 [4, 1, 14336, 4096], P(None, None, 'row', 'col'), may hold values from -250 to 250
- outer_left: bfloat16 [4, 1, 14336, 16], P(None, None, ('row', 'col')), may hold values from -6 to 6
- outer_right: bfloat16 [4, 1, 16, 4096], P(None, None, 'row', 'col'), may hold values from -12 to 12
- outer_mag: float32 [4, 1, 4096], P(None, None, 'col'), may hold values from 1792 to 7168
Outputs:
- inner_merged: bfloat16 [4, 1, 2, 4096, 14336], P(None, None, None, 'row', 'col')
- outer_merged: bfloat16 [4, 1, 14336, 4096], P(None, None, 'row', 'col')
The draws below stay inside these ranges and needn't reach their ends.
All inputs are finite; a program needn't handle non-finite values.
Results may differ from the reference program's by a relative error of at most 0.001.
Values may be sent and summed in bfloat16 or wider, within the bound.
A program may use at most 256 MiB of HBM per device.

```python
import math
import jax
import jax.numpy as jnp
from jax import lax

D = 4096
FF = 14336
RANK = 16
LAYERS = 4
EXPERTS = 1


def base_draw(key, extent):
    row_count = extent[-2]
    key_one, key_two = jax.random.split(key)
    scale_extent = extent[:-1] + (1,)
    jitter = jnp.clip(jax.random.normal(key_one, extent, jnp.float32), -6.0, 6.0)
    roughness = jnp.exp(jax.random.uniform(key_two, scale_extent, jnp.float32, 0.0, math.log(10.0)))
    growth = 2.0
    position = jnp.arange(row_count, dtype=jnp.float32) / max(row_count - 1, 1)
    rising = 1.0 + growth * position
    return (jitter * roughness * rising[:, None]).astype(jnp.bfloat16)


def draw_inner_base(key, part):
    return base_draw(jax.random.fold_in(key, 11), (LAYERS, EXPERTS, 2, D, FF))


def draw_outer_base(key, part):
    return base_draw(jax.random.fold_in(key, 23), (LAYERS, EXPERTS, FF, D))


def levels(rng, dims, pieces, least, top_value):
    level, own = 1.0, jax.random.fold_in(rng, 6)
    for dim, parts in pieces:
        steps = jnp.exp(jax.random.uniform(jax.random.fold_in(own, dim), (parts,), jnp.float32, least / len(pieces), top_value / len(pieces)))
        level = level * jnp.repeat(steps, dims[dim] // parts).reshape([-1 if axis == dim else 1 for axis in range(len(dims))])
    return level


def gaussian(key, dims, deviation, reach, pieces=(), kind=jnp.bfloat16):
    entries = deviation * jax.random.normal(key, dims, jnp.float32)
    if pieces:
        entries = entries * levels(key, dims, pieces, -0.22, 0.18)
    return jnp.clip(entries, -reach, reach).astype(kind)


def setup_inputs(seed: int = 0) -> dict:
    key_list = jax.random.split(jax.random.key(seed), 9)
    return {
        "inner_base": draw_inner_base(jax.random.fold_in(key_list[8], 71), 0),
        "inner_left": gaussian(key_list[1], (LAYERS, EXPERTS, 2, D, RANK), 1.0, 6.0, ((3, 32),)),
        "inner_right": gaussian(key_list[2], (LAYERS, EXPERTS, 2, RANK, FF), 2.0, 12.0, ((3, 4), (4, 8))),
        "inner_mag": jnp.clip(jnp.exp(math.log(2048.0) - 1.3862944 * jax.random.uniform(key_list[3], (LAYERS, EXPERTS, 2, FF), jnp.float32) ** levels(key_list[3], (LAYERS, EXPERTS, 2, FF), ((3, 8),), -0.2, 0.2)), 512.0, 2048.0),
        "outer_base": draw_outer_base(jax.random.fold_in(key_list[8], 71), 0),
        "outer_left": gaussian(key_list[5], (LAYERS, EXPERTS, FF, RANK), 1.0, 6.0, ((2, 32),)),
        "outer_right": gaussian(key_list[6], (LAYERS, EXPERTS, RANK, D), 2.0, 12.0, ((2, 4), (3, 8))),
        "outer_mag": jnp.clip(jnp.exp(math.log(7168.0) - 1.3862944 * jax.random.uniform(key_list[7], (LAYERS, EXPERTS, D), jnp.float32) ** levels(key_list[7], (LAYERS, EXPERTS, D), ((2, 8),), -0.2, 0.2)), 1792.0, 7168.0),
    }


epsilon = 1e-06

def merge_one(base, left, right, magnitude):
    delta = jnp.einsum('...ik,...kj->...ij', left.astype(jnp.float32), right.astype(jnp.float32))
    combined = base.astype(jnp.float32) + delta
    squares = lax.optimization_barrier(jnp.sum(combined * combined, axis=-2))
    factor = magnitude * lax.rsqrt(squares + epsilon)
    return (factor[..., None, :] * combined).astype(jnp.bfloat16)

def reference(inner_base, inner_left, inner_right, inner_mag, outer_base, outer_left, outer_right, outer_mag):
    inner_layers = []
    outer_layers = []
    for layer_index in range(LAYERS):
        inner_items = []
        outer_items = []
        for expert_index in range(EXPERTS):
            inner_items.append(merge_one(inner_base[layer_index, expert_index], inner_left[layer_index, expert_index], inner_right[layer_index, expert_index], inner_mag[layer_index, expert_index]))
            outer_items.append(merge_one(outer_base[layer_index, expert_index], outer_left[layer_index, expert_index], outer_right[layer_index, expert_index], outer_mag[layer_index, expert_index]))
        inner_layers.append(jnp.stack(inner_items))
        outer_layers.append(jnp.stack(outer_items))
    return (jnp.stack(inner_layers), jnp.stack(outer_layers))
```

```python
import functools

import jax
import jax.numpy as jnp
from jax import lax
from jax.experimental import pallas as pl
from jax.experimental.pallas import tpu as pltpu
from jax.sharding import PartitionSpec as P

epsilon = 1e-06
MESH = pl.DeviceIdType.MESH
ANY = pl.BlockSpec(memory_space=pl.ANY)
VMEM = pl.BlockSpec(memory_space=pltpu.VMEM)
GRANT = 18 << 20
SLOTS, PIECES = 4, 4


def peers_of(axis, n):
    me = lax.axis_index(axis)
    low, high, half = lax.rem(me, 2), lax.div(me, 2), n // 2
    partner = me + 1 - 2 * low
    ahead = [lax.rem(high + k, half) * 2 + low for k in range(1, half)]
    behind = [lax.rem(high + half - k, half) * 2 + low for k in range(1, half)]
    return me, partner, ahead, behind


def remote(src, dst, send, recv, axis, target):
    return pltpu.make_async_remote_copy(
        src_ref=src, dst_ref=dst, send_sem=send, recv_sem=recv, device_id={axis: target}, device_id_type=MESH
    )


def gather_kernel(rows, cols, il, ol, ir, orr, ib, ob, gil, gol, gir, gor, vib, vob, local, loads, send, recv):
    barrier = pltpu.get_barrier_semaphore()
    places = {"row": peers_of("row", rows), "col": peers_of("col", cols)}
    greeted = 0
    for axis, (_, partner, ahead, _) in places.items():
        for other in [partner, *ahead]:
            pl.semaphore_signal(barrier, inc=1, device_id={axis: other}, device_id_type=MESH)
            greeted += 1
    pl.semaphore_wait(barrier, greeted)
    items = [("row", rows, ir, gir), ("col", cols, il, gil), ("row", rows, orr, gor), ("col", cols, ol, gol)]
    sends, forwards, slot = [], [], 0
    for number, (axis, n, src, dst) in enumerate(items):
        me, partner, ahead, behind = places[axis]
        mine = pltpu.make_async_copy(src, dst.at[me], local.at[number])
        mine.start()
        arrivals = []
        for k, other in enumerate(ahead):
            copy = remote(src, dst.at[me], send.at[slot], recv.at[slot], axis, other)
            copy.start()
            sends.append(copy)
            arrivals.append((slot, behind[k]))
            slot += 1
        copy = remote(src, dst.at[me], send.at[slot], recv.at[slot], axis, partner)
        copy.start()
        sends.append(copy)
        forwards.append((copy, mine))
        slot += 1
        items[number] = (axis, dst, partner, arrivals)
    bases = []
    for number, (src, dst) in enumerate(((ib, vib), (ob, vob))):
        for t in range(src.shape[0]):
            copy = pltpu.make_async_copy(src.at[t], dst.at[t], loads.at[len(bases)])
            copy.start()
            bases.append(copy)
    last = [f for f, _ in forwards]
    for axis, dst, partner, arrivals in items:
        for number, source in arrivals:
            remote(dst.at[source], dst.at[source], send.at[number], recv.at[number], axis, partner).wait_recv()
            copy = remote(dst.at[source], dst.at[source], send.at[slot], recv.at[slot], axis, partner)
            copy.start()
            sends.append(copy)
            last.append(copy)
            slot += 1
    for copy in last:
        copy.wait_recv()
    for copy in sends:
        copy.wait_send()
    for _, mine in forwards:
        mine.wait()
    for copy in bases:
        copy.wait()


def prepare(left, right, lt, r32, t, rank):
    pieces, _, _, piece = left.shape
    for c in range(pieces):
        lt[c * piece : (c + 1) * piece, :] = left[c, t].T
    for c in range(right.shape[0]):
        share = right.shape[2]
        r32[c * share : (c + 1) * share, :] = right[c, t].astype(jnp.float32)


def tiles(rows, cols):
    width = 256 if cols % 256 == 0 else 128 if cols % 128 == 0 else cols
    height = next(h for h in (256, 128, 64, 32, 16) if rows % h == 0)
    return height, width


def squares_weight(left, right, base, out, lt, r32, r16, acc):
    count, rows, cols = base.shape
    height, width = tiles(rows, cols)

    @pl.loop(0, count)
    def _(t):
        prepare(left, right, lt, r32, t, r32.shape[0])
        r16[...] = r32[...].astype(jnp.bfloat16)
        for j in range(cols // width):
            part = slice(j * width, (j + 1) * width)

            def add(i, total):
                span = pl.ds(pl.multiple_of(i * height, height), height)
                delta = jnp.dot(lt[span, :], r16[:, part], preferred_element_type=jnp.float32)
                full = base[t, span, part].astype(jnp.float32) + delta
                return total + jnp.sum((full * full).reshape(height // 8, 8, width), axis=0)

            total = lax.fori_loop(0, rows // height, add, jnp.zeros((8, width), jnp.float32))
            acc[:, part] = total
        out[t] = jnp.sum(acc[...], axis=0, keepdims=True)


def squares_kernel(gil, gol, gir, gor, vib, vob, sin, sout, lti, lto, r32i, r32o, r16i, r16o, acci, acco):
    squares_weight(gil, gir, vib, sin, lti, r32i, r16i, acci)
    squares_weight(gol, gor, vob, sout, lto, r32o, r16o, acco)


def factor_kernel(rows, sin, sout, min_, mout, fin, fout, hin, hout, send, recv):
    me = lax.axis_index("row")
    barrier = pltpu.get_barrier_semaphore()
    others = [lax.rem(me + k, rows) for k in range(1, rows)]
    for other in others:
        pl.semaphore_signal(barrier, inc=1, device_id={"row": other}, device_id_type=MESH)
    pl.semaphore_wait(barrier, rows - 1)
    copies = []
    for k, other in enumerate(others):
        for number, (src, held) in enumerate(((sin, hin), (sout, hout))):
            slot = 2 * k + number
            copy = remote(src, held.at[k], send.at[slot], recv.at[slot], "row", other)
            copy.start()
            copies.append(copy)
    for copy in copies:
        copy.wait()
    for src, held, mag, out in ((sin, hin, min_, fin), (sout, hout, mout, fout)):
        total = src[...]
        for k in range(rows - 1):
            total = total + held[k]
        scale = lax.rsqrt(total + epsilon)
        groups = mag.shape[1]
        for t in range(out.shape[0]):
            row = t % groups
            out[t] = mag[t // groups, row : row + 1, :] * scale[t]


def scale_weight(left, right, base, factor, out, lt, r32, r16, stage, sems):
    count, rows, cols = base.shape
    slots, chunk, _ = stage.shape
    pieces = rows // chunk
    height, width = tiles(chunk, cols)

    def store(step):
        slot = lax.rem(step, slots)
        span = pl.ds(pl.multiple_of(lax.rem(step, pieces) * chunk, chunk), chunk)
        return pltpu.make_async_copy(stage.at[slot], out.at[lax.div(step, pieces), span], sems.at[slot])

    @pl.loop(0, count)
    def _(t):
        prepare(left, right, lt, r32, t, r32.shape[0])
        r16[...] = r32[...].astype(jnp.bfloat16)

        @pl.loop(0, pieces)
        def _(p):
            step = t * pieces + p
            slot = lax.rem(step, slots)

            @pl.when(step >= slots)
            def _():
                store(step - slots).wait()

            for j in range(cols // width):
                part = slice(j * width, (j + 1) * width)
                scale = jnp.broadcast_to(factor[t, :, part], (8, width))

                def merge(i, carry):
                    span = pl.ds(pl.multiple_of(p * chunk + i * height, height), height)
                    delta = jnp.dot(lt[span, :], r16[:, part], preferred_element_type=jnp.float32)
                    full = base[t, span, part].astype(jnp.float32) + delta
                    merged = full.reshape(height // 8, 8, width) * scale[None]
                    local = pl.ds(pl.multiple_of(i * height, height), height)
                    stage[slot, local, part] = merged.reshape(height, width).astype(jnp.bfloat16)
                    return carry

                lax.fori_loop(0, chunk // height, merge, 0)
            store(step).start()

    return [store(step) for step in range(count * pieces - slots, count * pieces)]


def scale_kernel(
    gil, gol, gir, gor, vib, vob, fin, fout, oin, oout, lti, lto, r32i, r32o, r16i, r16o, stagei, stageo, semi, semo
):
    stores = scale_weight(gil, gir, vib, fin, oin, lti, r32i, r16i, stagei, semi)
    stores += scale_weight(gol, gor, vob, fout, oout, lto, r32o, r16o, stageo, semo)
    for copy in stores:
        copy.wait()


def pinned(arrays):
    return [pltpu.with_memory_space_constraint(a, pltpu.VMEM) for a in arrays]


def shards(rows, cols, inner_base, inner_left, inner_right, inner_mag, outer_base, outer_left, outer_right, outer_mag):
    rank = inner_left.shape[-1]
    ib = inner_base.reshape((-1, *inner_base.shape[-2:]))
    ob = outer_base.reshape((-1, *outer_base.shape[-2:]))
    il = jnp.swapaxes(inner_left, -1, -2).reshape((-1, rank, inner_left.shape[-2]))
    ol = jnp.swapaxes(outer_left, -1, -2).reshape((-1, rank, outer_left.shape[-2]))
    ir = inner_right.reshape((-1, *inner_right.shape[-2:]))
    orr = outer_right.reshape((-1, *outer_right.shape[-2:]))
    im = inner_mag.reshape((-1, *inner_mag.shape[-2:]))
    om = outer_mag.reshape((ob.shape[0], 1, -1))
    weights, bf16, f32 = ib.shape[0] + ob.shape[0], jnp.bfloat16, jnp.float32
    copies = 4 * (cols + rows)
    gathered = pl.pallas_call(
        functools.partial(gather_kernel, rows, cols),
        out_shape=[
            pltpu.VMEM((n, *a.shape), bf16) for n, a in ((cols, il), (cols, ol), (rows, ir), (rows, orr))
        ] + [pltpu.VMEM(a.shape, bf16) for a in (ib, ob)],
        in_specs=[ANY] * 6,
        out_specs=[VMEM] * 6,
        scratch_shapes=[
            pltpu.SemaphoreType.DMA((4,)),
            pltpu.SemaphoreType.DMA((weights,)),
            pltpu.SemaphoreType.DMA((copies,)),
            pltpu.SemaphoreType.DMA((copies,)),
        ],
        compiler_params=pltpu.CompilerParams(collective_id=0, has_side_effects=True, vmem_limit_bytes=GRANT),
        name="gather",
    )(il, ol, ir, orr, ib, ob)
    gathered = pinned(gathered)
    work = []
    for shape in ((ib.shape[1], rank), (ob.shape[1], rank)):
        work.append(pltpu.VMEM(shape, bf16))
    for kind in (f32, bf16):
        for base in (ib, ob):
            work.append(pltpu.VMEM((rank, base.shape[2]), kind))
    sums = pl.pallas_call(
        squares_kernel,
        out_shape=[pltpu.VMEM((a.shape[0], 1, a.shape[2]), f32) for a in (ib, ob)],
        in_specs=[VMEM] * 6,
        out_specs=[VMEM] * 2,
        scratch_shapes=work + [pltpu.VMEM((8, a.shape[2]), f32) for a in (ib, ob)],
        compiler_params=pltpu.CompilerParams(vmem_limit_bytes=GRANT),
        name="squares",
    )(*gathered)
    sums = pinned(sums)
    factors = pl.pallas_call(
        functools.partial(factor_kernel, rows),
        out_shape=[pltpu.VMEM(s.shape, f32) for s in sums],
        in_specs=[VMEM] * 4,
        out_specs=[VMEM] * 2,
        scratch_shapes=[pltpu.VMEM((rows - 1, *s.shape), f32) for s in sums]
        + [pltpu.SemaphoreType.DMA((2 * rows - 2,))] * 2,
        compiler_params=pltpu.CompilerParams(collective_id=1, has_side_effects=True, vmem_limit_bytes=GRANT),
        name="factor",
    )(*sums, im, om)
    inner, outer = pl.pallas_call(
        scale_kernel,
        out_shape=[jax.ShapeDtypeStruct(a.shape, bf16) for a in (ib, ob)],
        in_specs=[VMEM] * 8,
        out_specs=[ANY] * 2,
        scratch_shapes=work
        + [pltpu.VMEM((SLOTS, a.shape[1] // PIECES, a.shape[2]), bf16) for a in (ib, ob)]
        + [pltpu.SemaphoreType.DMA((SLOTS,))] * 2,
        compiler_params=pltpu.CompilerParams(vmem_limit_bytes=GRANT),
        name="scale",
    )(*gathered, *pinned(factors))
    return inner.reshape(inner_base.shape), outer.reshape(outer_base.shape)


def solution(mesh):
    in_specs = (
        P(None, None, None, "row", "col"),
        P(None, None, None, ("row", "col"), None),
        P(None, None, None, "row", "col"),
        P(None, None, None, "col"),
        P(None, None, "row", "col"),
        P(None, None, ("row", "col"), None),
        P(None, None, "row", "col"),
        P(None, None, "col"),
    )
    out_specs = (P(None, None, None, "row", "col"), P(None, None, "row", "col"))
    body = functools.partial(shards, mesh.shape["row"], mesh.shape["col"])
    return jax.shard_map(body, mesh=mesh, in_specs=in_specs, out_specs=out_specs, check_vma=False)
```

```python
import functools

import jax
import jax.numpy as jnp
from jax import lax
from jax.experimental import pallas as pl
from jax.experimental.pallas import tpu as pltpu
from jax.sharding import PartitionSpec as P

epsilon = 1e-06
MESH = pl.DeviceIdType.MESH
ANY = pl.BlockSpec(memory_space=pl.ANY)
VMEM = pl.BlockSpec(memory_space=pltpu.VMEM)
GRANT = 18 << 20
SLOTS, PIECES = 4, 2
WIDTHS = (256, 128)
HEIGHTS = (512, 896, 256, 128, 64, 32, 16)


def peers_of(axis, n):
    me = lax.axis_index(axis)
    low, high, half = lax.rem(me, 2), lax.div(me, 2), n // 2
    partner = me + 1 - 2 * low
    ahead = [lax.rem(high + k, half) * 2 + low for k in range(1, half)]
    behind = [lax.rem(high + half - k, half) * 2 + low for k in range(1, half)]
    return me, partner, ahead, behind


def remote(src, dst, send, recv, axis, target):
    return pltpu.make_async_remote_copy(
        src_ref=src, dst_ref=dst, send_sem=send, recv_sem=recv, device_id={axis: target}, device_id_type=MESH
    )


def gather_kernel(rows, cols, il, ol, ir, orr, ib, ob, gil, gol, gir, gor, vib, vob, local, loads, send, recv):
    barrier = pltpu.get_barrier_semaphore()
    places = {"row": peers_of("row", rows), "col": peers_of("col", cols)}
    greeted = 0
    for axis, (_, partner, ahead, _) in places.items():
        for other in [partner, *ahead]:
            pl.semaphore_signal(barrier, inc=1, device_id={axis: other}, device_id_type=MESH)
            greeted += 1
    pl.semaphore_wait(barrier, greeted)
    items = [("row", rows, ir, gir), ("col", cols, il, gil), ("row", rows, orr, gor), ("col", cols, ol, gol)]
    sends, forwards, slot = [], [], 0
    for number, (axis, n, src, dst) in enumerate(items):
        me, partner, ahead, behind = places[axis]
        mine = pltpu.make_async_copy(src, dst.at[me], local.at[number])
        mine.start()
        arrivals = []
        for k, other in enumerate(ahead):
            copy = remote(src, dst.at[me], send.at[slot], recv.at[slot], axis, other)
            copy.start()
            sends.append(copy)
            arrivals.append((slot, behind[k]))
            slot += 1
        copy = remote(src, dst.at[me], send.at[slot], recv.at[slot], axis, partner)
        copy.start()
        sends.append(copy)
        forwards.append((copy, mine))
        slot += 1
        items[number] = (axis, dst, partner, arrivals)
    bases = []
    for number, (src, dst) in enumerate(((ib, vib), (ob, vob))):
        for t in range(src.shape[0]):
            copy = pltpu.make_async_copy(src.at[t], dst.at[t], loads.at[len(bases)])
            copy.start()
            bases.append(copy)
    last = [f for f, _ in forwards]
    for axis, dst, partner, arrivals in items:
        for number, source in arrivals:
            remote(dst.at[source], dst.at[source], send.at[number], recv.at[number], axis, partner).wait_recv()
            copy = remote(dst.at[source], dst.at[source], send.at[slot], recv.at[slot], axis, partner)
            copy.start()
            sends.append(copy)
            last.append(copy)
            slot += 1
    for copy in last:
        copy.wait_recv()
    for copy in sends:
        copy.wait_send()
    for _, mine in forwards:
        mine.wait()
    for copy in bases:
        copy.wait()


def prepare(left, right, lt, r32, t, rank):
    pieces, _, _, piece = left.shape
    for c in range(pieces):
        lt[c * piece : (c + 1) * piece, :] = left[c, t].T
    for c in range(right.shape[0]):
        share = right.shape[2]
        r32[c * share : (c + 1) * share, :] = right[c, t].astype(jnp.float32)


def tiles(rows, cols):
    width = next((w for w in WIDTHS if cols % w == 0), cols)
    height = next(h for h in HEIGHTS if rows % h == 0)
    return height, width


def squares_weight(left, right, base, out, lt, r32, r16, acc):
    count, rows, cols = base.shape
    height, width = tiles(rows, cols)

    @pl.loop(0, count)
    def _(t):
        prepare(left, right, lt, r32, t, r32.shape[0])
        r16[...] = r32[...].astype(jnp.bfloat16)
        for j in range(cols // width):
            part = slice(j * width, (j + 1) * width)

            def add(i, total):
                span = pl.ds(pl.multiple_of(i * height, height), height)
                delta = jnp.dot(lt[span, :], r16[:, part], preferred_element_type=jnp.float32)
                full = base[t, span, part].astype(jnp.float32) + delta
                return total + jnp.sum((full * full).reshape(height // 8, 8, width), axis=0)

            total = lax.fori_loop(0, rows // height, add, jnp.zeros((8, width), jnp.float32), unroll=True)
            acc[:, part] = total
        out[t] = jnp.sum(acc[...], axis=0, keepdims=True)


def squares_kernel(gil, gol, gir, gor, vib, vob, sin, sout, lti, lto, r32i, r32o, r16i, r16o, acci, acco):
    squares_weight(gil, gir, vib, sin, lti, r32i, r16i, acci)
    squares_weight(gol, gor, vob, sout, lto, r32o, r16o, acco)


def factor_kernel(rows, sin, sout, min_, mout, fin, fout, hin, hout, send, recv):
    me = lax.axis_index("row")
    barrier = pltpu.get_barrier_semaphore()
    others = [lax.rem(me + k, rows) for k in range(1, rows)]
    for other in others:
        pl.semaphore_signal(barrier, inc=1, device_id={"row": other}, device_id_type=MESH)
    pl.semaphore_wait(barrier, rows - 1)
    copies = []
    for k, other in enumerate(others):
        for number, (src, held) in enumerate(((sin, hin), (sout, hout))):
            slot = 2 * k + number
            copy = remote(src, held.at[k], send.at[slot], recv.at[slot], "row", other)
            copy.start()
            copies.append(copy)
    for copy in copies:
        copy.wait()
    for src, held, mag, out in ((sin, hin, min_, fin), (sout, hout, mout, fout)):
        total = src[...]
        for k in range(rows - 1):
            total = total + held[k]
        scale = lax.rsqrt(total + epsilon)
        groups = mag.shape[1]
        for t in range(out.shape[0]):
            row = t % groups
            out[t] = mag[t // groups, row : row + 1, :] * scale[t]


def scale_weight(left, right, base, factor, out, lt, r32, r16, stage, sems):
    count, rows, cols = base.shape
    slots, chunk, _ = stage.shape
    pieces = rows // chunk
    height, width = tiles(chunk, cols)

    def store(step):
        slot = lax.rem(step, slots)
        span = pl.ds(pl.multiple_of(lax.rem(step, pieces) * chunk, chunk), chunk)
        return pltpu.make_async_copy(stage.at[slot], out.at[lax.div(step, pieces), span], sems.at[slot])

    @pl.loop(0, count)
    def _(t):
        prepare(left, right, lt, r32, t, r32.shape[0])
        r16[...] = r32[...].astype(jnp.bfloat16)

        @pl.loop(0, pieces)
        def _(p):
            step = t * pieces + p
            slot = lax.rem(step, slots)

            @pl.when(step >= slots)
            def _():
                store(step - slots).wait()

            for j in range(cols // width):
                part = slice(j * width, (j + 1) * width)
                scale = jnp.broadcast_to(factor[t, :, part], (8, width))

                def merge(i, carry):
                    span = pl.ds(pl.multiple_of(p * chunk + i * height, height), height)
                    delta = jnp.dot(lt[span, :], r16[:, part], preferred_element_type=jnp.float32)
                    full = base[t, span, part].astype(jnp.float32) + delta
                    merged = full.reshape(height // 8, 8, width) * scale[None]
                    local = pl.ds(pl.multiple_of(i * height, height), height)
                    stage[slot, local, part] = merged.reshape(height, width).astype(jnp.bfloat16)
                    return carry

                lax.fori_loop(0, chunk // height, merge, 0, unroll=True)
            store(step).start()

    return [store(step) for step in range(count * pieces - slots, count * pieces)]


def scale_kernel(
    gil, gol, gir, gor, vib, vob, fin, fout, oin, oout, lti, lto, r32i, r32o, r16i, r16o, stagei, stageo, semi, semo
):
    stores = scale_weight(gil, gir, vib, fin, oin, lti, r32i, r16i, stagei, semi)
    stores += scale_weight(gol, gor, vob, fout, oout, lto, r32o, r16o, stageo, semo)
    for copy in stores:
        copy.wait()


def pinned(arrays):
    return [pltpu.with_memory_space_constraint(a, pltpu.VMEM) for a in arrays]


def shards(rows, cols, inner_base, inner_left, inner_right, inner_mag, outer_base, outer_left, outer_right, outer_mag):
    rank = inner_left.shape[-1]
    ib = inner_base.reshape((-1, *inner_base.shape[-2:]))
    ob = outer_base.reshape((-1, *outer_base.shape[-2:]))
    il = jnp.swapaxes(inner_left, -1, -2).reshape((-1, rank, inner_left.shape[-2]))
    ol = jnp.swapaxes(outer_left, -1, -2).reshape((-1, rank, outer_left.shape[-2]))
    ir = inner_right.reshape((-1, *inner_right.shape[-2:]))
    orr = outer_right.reshape((-1, *outer_right.shape[-2:]))
    im = inner_mag.reshape((-1, *inner_mag.shape[-2:]))
    om = outer_mag.reshape((ob.shape[0], 1, -1))
    weights, bf16, f32 = ib.shape[0] + ob.shape[0], jnp.bfloat16, jnp.float32
    copies = 4 * (cols + rows)
    gathered = pl.pallas_call(
        functools.partial(gather_kernel, rows, cols),
        out_shape=[
            pltpu.VMEM((n, *a.shape), bf16) for n, a in ((cols, il), (cols, ol), (rows, ir), (rows, orr))
        ] + [pltpu.VMEM(a.shape, bf16) for a in (ib, ob)],
        in_specs=[ANY] * 6,
        out_specs=[VMEM] * 6,
        scratch_shapes=[
            pltpu.SemaphoreType.DMA((4,)),
            pltpu.SemaphoreType.DMA((weights,)),
            pltpu.SemaphoreType.DMA((copies,)),
            pltpu.SemaphoreType.DMA((copies,)),
        ],
        compiler_params=pltpu.CompilerParams(collective_id=0, has_side_effects=True, vmem_limit_bytes=GRANT),
        name="gather",
    )(il, ol, ir, orr, ib, ob)
    gathered = pinned(gathered)
    work = []
    for shape in ((ib.shape[1], rank), (ob.shape[1], rank)):
        work.append(pltpu.VMEM(shape, bf16))
    for kind in (f32, bf16):
        for base in (ib, ob):
            work.append(pltpu.VMEM((rank, base.shape[2]), kind))
    sums = pl.pallas_call(
        squares_kernel,
        out_shape=[pltpu.VMEM((a.shape[0], 1, a.shape[2]), f32) for a in (ib, ob)],
        in_specs=[VMEM] * 6,
        out_specs=[VMEM] * 2,
        scratch_shapes=work + [pltpu.VMEM((8, a.shape[2]), f32) for a in (ib, ob)],
        compiler_params=pltpu.CompilerParams(vmem_limit_bytes=GRANT),
        name="squares",
    )(*gathered)
    sums = pinned(sums)
    factors = pl.pallas_call(
        functools.partial(factor_kernel, rows),
        out_shape=[pltpu.VMEM(s.shape, f32) for s in sums],
        in_specs=[VMEM] * 4,
        out_specs=[VMEM] * 2,
        scratch_shapes=[pltpu.VMEM((rows - 1, *s.shape), f32) for s in sums]
        + [pltpu.SemaphoreType.DMA((2 * rows - 2,))] * 2,
        compiler_params=pltpu.CompilerParams(collective_id=1, has_side_effects=True, vmem_limit_bytes=GRANT),
        name="factor",
    )(*sums, im, om)
    inner, outer = pl.pallas_call(
        scale_kernel,
        out_shape=[jax.ShapeDtypeStruct(a.shape, bf16) for a in (ib, ob)],
        in_specs=[VMEM] * 8,
        out_specs=[ANY] * 2,
        scratch_shapes=work
        + [pltpu.VMEM((SLOTS, a.shape[1] // PIECES, a.shape[2]), bf16) for a in (ib, ob)]
        + [pltpu.SemaphoreType.DMA((SLOTS,))] * 2,
        compiler_params=pltpu.CompilerParams(vmem_limit_bytes=GRANT),
        name="scale",
    )(*gathered, *pinned(factors))
    return inner.reshape(inner_base.shape), outer.reshape(outer_base.shape)


def solution(mesh):
    in_specs = (
        P(None, None, None, "row", "col"),
        P(None, None, None, ("row", "col"), None),
        P(None, None, None, "row", "col"),
        P(None, None, None, "col"),
        P(None, None, "row", "col"),
        P(None, None, ("row", "col"), None),
        P(None, None, "row", "col"),
        P(None, None, "col"),
    )
    out_specs = (P(None, None, None, "row", "col"), P(None, None, "row", "col"))
    body = functools.partial(shards, mesh.shape["row"], mesh.shape["col"])
    return jax.shard_map(body, mesh=mesh, in_specs=in_specs, out_specs=out_specs, check_vma=False)
```
